32 devices in a mesh: wide: 8 (over z, x), narrow: 4 (over y, core).
Axes of the slice: x: 2, y: 2, z: 4, core: 2. Of those that a mesh axis runs over, the one named last changes fastest.
Arguments:
- harvest: bfloat16 [128, 16384], P('wide', 'narrow'), may hold values from -6 to 6
- pair_ids: int32 [16], P('wide'), may hold values from 0 to 15
- w_enc: bfloat16 [16384, 32768], P('narrow', 'wide'), may hold values from -0.046875 to 0.046875
- b_enc: float32 [32768], P('wide'), may hold values from -3 to 3
- w_dec: bfloat16 [32768, 16384], P('wide', 'narrow'), may hold values from -0.03125 to 0.03125
- b_dec: float32 [16384], P('narrow'), may hold values from -3 to 3
- step_size: float32 [], replicated, may hold values from 0.1 to 0.33
- penalty: float32 [], replicated, may hold values from 0.5 to 2
Outputs:
- latents: float32 [16, 32768], P(None, 'wide')
The draws below stay inside these ranges and needn't reach their ends.
Inputs may be any that keep to these rules, and one draw needn't show every extreme that they name: Token pair b takes pool row (b // 2) * 16 + pair_ids[b].
All inputs are finite; a program needn't handle non-finite values.
Results may differ from the reference program's by a relative error of at most 0.0025.
Values may be sent and summed in bfloat16 or wider, within the bound.
No kernel may reach another device: no remote copies, remote signals or barrier semaphores. Data moves between devices by JAX's collectives and lax.ppermute only.
A program may use at most 128 MiB of HBM per device.

```python
import jax
import jax.numpy as jnp
from jax import lax

MODEL_D = 8192
D = 16384
LAT = 32768
ITERS = 2
ROWS_DEV = 2
POOL_DEV = 16
BATCH = 16
POOL = 128


def with_ends(result, stream_key, low, high):
    longest = result.shape.index(max(result.shape))
    spots = []
    for shift in (0, 1):
        where = [jax.random.randint(jax.random.fold_in(stream_key, axis), (), 0, length) for axis, length in enumerate(result.shape)]
        where[longest] = (where[longest] + shift) % result.shape[longest]
        spots.append(tuple(where))
    return result.at[spots[0]].set(low).at[spots[1]].set(high)


def block_levels(own_key, shape, cuts, smallest, top_value):
    factor_of, own = 1.0, jax.random.fold_in(own_key, 6)
    for axis_at, blocks in cuts:
        steps = jnp.exp(jax.random.uniform(jax.random.fold_in(own, axis_at), (blocks,), jnp.float32, smallest / len(cuts), top_value / len(cuts)))
        factor_of = factor_of * jnp.repeat(steps, shape[axis_at] // blocks).reshape([-1 if axis == axis_at else 1 for axis in range(len(shape))])
    return factor_of


def scatter_about(own_key, dims, spread, most, pieces=(), held_as=jnp.bfloat16):
    drawn = jax.random.normal(own_key, dims, jnp.float32) * spread
    if len(pieces) > 0:
        drawn = block_levels(own_key, dims, pieces, -0.22, 0.18) * drawn
    return jnp.clip(drawn, min=-most, max=most).astype(held_as)


def setup_inputs(seed: int = 0) -> dict:
    key_list = jax.random.split(jax.random.key(seed), 9)
    return {
        "harvest": scatter_about(key_list[0], (POOL, D), 1.0, 6.0, ((0, 8), (1, 4))),
        "pair_ids": with_ends(jax.random.randint(key_list[1], (BATCH,), 0, POOL_DEV), jax.random.fold_in(key_list[1], 1), 0, POOL_DEV - 1).astype(jnp.int32),
        "w_enc": scatter_about(key_list[2], (D, LAT), D ** -0.5, 0.046875, ((0, 4), (1, 8))),
        "b_enc": scatter_about(key_list[3], (LAT,), 0.5, 3.0, ((0, 8),), jnp.float32),
        "w_dec": scatter_about(key_list[4], (LAT, D), LAT ** -0.5, 0.03125, ((0, 8), (1, 4))),
        "b_dec": scatter_about(key_list[5], (D,), 0.5, 3.0, ((0, 4),), jnp.float32),
        "step_size": jnp.clip(jax.random.uniform(key_list[6], (), jnp.float32, 0.1, 0.33), 0.1, 0.33),
        "penalty": jnp.clip(jax.random.uniform(key_list[7], (), jnp.float32, 0.5, 2.0), 0.5, 2.0),
    }


def reference(harvest, pair_ids, w_enc, b_enc, w_dec, b_dec, step_size, penalty):
    index_rows = jnp.arange(BATCH, dtype=jnp.int32) // ROWS_DEV * POOL_DEV + pair_ids.astype(jnp.int32)
    pairs = jnp.take(harvest, index_rows, axis=0)
    pre = jnp.dot(pairs, w_enc, preferred_element_type=jnp.float32)
    decoder = w_dec.astype(jnp.float32)
    norm_base = jnp.sqrt(lax.optimization_barrier(jnp.sum(decoder[:, :MODEL_D] * decoder[:, :MODEL_D], axis=1)))
    norm_inst = jnp.sqrt(lax.optimization_barrier(jnp.sum(decoder[:, MODEL_D:] * decoder[:, MODEL_D:], axis=1)))
    thresh = penalty * step_size * (norm_base + norm_inst)
    latents = jnp.maximum(pre + b_enc, 0.0)
    for step in range(ITERS):
        codes = latents.astype(jnp.bfloat16)
        rebuilt = jnp.dot(codes, w_dec, preferred_element_type=jnp.float32)
        residual = (pairs.astype(jnp.float32) - rebuilt - b_dec).astype(jnp.bfloat16)
        grad = jnp.dot(residual, w_dec.T, preferred_element_type=jnp.float32)
        latents = jnp.maximum(latents + step_size * grad - thresh, 0.0)
    return latents
```

```python
import functools

import jax
import jax.numpy as jnp
from jax import lax
from jax.experimental import pallas as pl
from jax.experimental.pallas import tpu as pltpu
from jax.sharding import PartitionSpec as P

ITERS = 2
MIB = 1024 * 1024
F32 = jnp.float32
BF16 = jnp.bfloat16
NT = (((1,), (1,)), ((), ()))


def swap(value, axis, distance):
    pairs = [(i, i ^ distance) for i in range(lax.axis_size(axis))]
    return lax.ppermute(value, axis, pairs)


def bits_of(axis):
    size = lax.axis_size(axis)
    assert size & (size - 1) == 0
    return [1 << k for k in range(size.bit_length() - 1)]


def tile_of(length, most):
    size = most
    while length % size:
        size //= 2
    return size


def half_start(axis, bit, half, other):
    high = jnp.where((lax.axis_index(axis) & bit) != 0, 1, 0)
    start = (1 - high if other else high) * half
    return pl.multiple_of(start, half)


def local_call(body, name, arrays, outs, flops, scalars=(), scratch=(), vmem=16, in_hbm=(), traffic=None):
    specs = [pl.BlockSpec(memory_space=pltpu.SMEM)] * len(scalars)
    specs += [pl.BlockSpec(memory_space=pltpu.HBM if k in in_hbm else pltpu.VMEM) for k in range(len(arrays))]
    multiple = isinstance(outs, (list, tuple))
    out_spec = pl.BlockSpec(memory_space=pltpu.VMEM)
    return pl.pallas_call(
        body,
        out_shape=outs,
        in_specs=specs,
        out_specs=[out_spec] * len(outs) if multiple else out_spec,
        scratch_shapes=list(scratch),
        compiler_params=pltpu.CompilerParams(vmem_limit_bytes=vmem * MIB),
        cost_estimate=pl.CostEstimate(flops=flops, bytes_accessed=flops // 32 if traffic is None else traffic, transcendentals=0),
        name=name,
    )(*scalars, *arrays)


def select(harvest, pair_ids, step_size, penalty, half_lat, w_enc):
    pool, feat = harvest.shape
    rows = pair_ids.shape[0]

    def body(step_ref, pen_ref, ids_ref, pool_ref, _, o_ref, step_row, pen_row):
        row = lax.broadcasted_iota(jnp.int32, (rows, pool), 0)
        col = lax.broadcasted_iota(jnp.int32, (rows, pool), 1)
        taken = jnp.zeros((rows, pool), F32)
        for r in range(rows):
            taken = jnp.where((row == r) & (col == ids_ref[r]), 1.0, taken)
        taken = taken.astype(BF16)
        chunk = tile_of(feat, 1024)

        @pl.loop(0, feat // chunk)
        def _(j):
            here = pl.ds(pl.multiple_of(j * chunk, chunk), chunk)
            o_ref[:, here] = jnp.dot(taken, pool_ref[:, here], preferred_element_type=F32).astype(BF16)

        step_row[...] = jnp.full((1, half_lat), step_ref[0, 0], F32)
        pen_row[...] = jnp.full((1, half_lat), pen_ref[0, 0] * step_ref[0, 0], F32)

    outs = [
        jax.ShapeDtypeStruct((rows, feat), BF16),
        jax.ShapeDtypeStruct((1, half_lat), F32),
        jax.ShapeDtypeStruct((1, half_lat), F32),
    ]
    scalars = [step_size.reshape(1, 1), penalty.reshape(1, 1), pair_ids]
    return local_call(body, "select", [harvest, w_enc], outs, 1 << 20, scalars, vmem=4, in_hbm=(1,))


def merge(mine, other, w_enc):
    count, feat = mine.shape

    def body(mine_ref, other_ref, _, o_ref):
        both = jnp.concatenate([mine_ref[...].astype(F32), other_ref[...].astype(F32)])
        o_ref[...] = both.astype(BF16)

    out = jax.ShapeDtypeStruct((2 * count, feat), BF16)
    return local_call(body, "merge", [mine, other, w_enc], out, 1 << 20, vmem=4, in_hbm=(2,))


def hold(w_dec, after):
    def body(w_ref, after_ref, o_ref):
        o_ref[...] = jnp.zeros(o_ref.shape, F32)

    out = jax.ShapeDtypeStruct((8, 128), F32)
    return local_call(body, "hold", [w_dec, pltpu.with_memory_space_constraint(after, pltpu.HBM)], out, 1 << 10, in_hbm=(1,))


def order(mine, other, b_enc, b_dec, step_row, pen_row, held, rows, far, hidden):
    count, feat = mine.shape
    half_feat, half_lat = feat // 2, b_enc.shape[1] // 2

    def body(mine_ref, other_ref, b_enc_ref, b_dec_ref, step_ref, pen_ref, _, all_ref, own_ref, enc_ref, dec_ref, step_out, pen_out):
        me = lax.axis_index("wide")
        row = lax.broadcasted_iota(jnp.int32, (2 * count, count), 0)
        col = lax.broadcasted_iota(jnp.int32, (2 * count, count), 1)

        def place(base):
            at = col + base
            return (row == rows * (me ^ (at // rows)) + at % rows).astype(F32).astype(BF16)

        chunk = tile_of(half_feat, 1024)
        start = half_start("wide", hidden, half_feat, False)

        @pl.loop(0, feat // chunk)
        def _(j):
            here = pl.ds(pl.multiple_of(j * chunk, chunk), chunk)
            both = jnp.dot(place(0), mine_ref[:, here], preferred_element_type=F32)
            both = both + jnp.dot(place(count), other_ref[:, here], preferred_element_type=F32)
            all_ref[:, here] = both.astype(BF16)

        own_ref[...] = all_ref[:, pl.ds(start, half_feat)]
        dec_ref[...] = b_dec_ref[:, pl.ds(start, half_feat)]
        enc_ref[...] = b_enc_ref[:, pl.ds(half_start("narrow", far, half_lat, False), half_lat)]
        step_out[...] = step_ref[...]
        pen_out[...] = pen_ref[...]

    outs = [
        jax.ShapeDtypeStruct((2 * count, feat), BF16),
        jax.ShapeDtypeStruct((2 * count, half_feat), BF16),
        jax.ShapeDtypeStruct((1, half_lat), F32),
        jax.ShapeDtypeStruct((1, half_feat), F32),
        jax.ShapeDtypeStruct((1, half_lat), F32),
        jax.ShapeDtypeStruct((1, half_lat), F32),
    ]
    return local_call(body, "order", [mine, other, b_enc, b_dec, step_row, pen_row, held], outs, 1 << 20, vmem=4)


def pointwise(fn, name, arrays, outs, w_dec):
    def body(*refs):
        ins, out_refs = refs[:len(arrays)], refs[len(arrays) + 1:]
        values = fn(*(ref[...] for ref in ins))
        for ref, value in zip(out_refs, values, strict=True):
            ref[...] = value

    return local_call(body, name, [*arrays, w_dec], outs, 1 << 16)


def encode(x, w, far, other, name):
    depth, lat = w.shape
    half = lat // 2
    chunk = tile_of(depth, 512)
    steps = depth // chunk
    slots = min(4, steps)

    def body(x_ref, w_ref, o_ref, held, sems):
        start = half_start("narrow", far, half, other)

        def fetch(k):
            return pltpu.make_async_copy(
                w_ref.at[pl.ds(k * chunk, chunk), pl.ds(start, half)], held.at[k % slots], sems.at[k % slots]
            )

        for k in range(slots):
            fetch(k).start()
        for k in range(steps):
            fetch(k).wait()
            width = tile_of(half, 1024)

            @pl.loop(0, half // width)
            def _(j):
                here = pl.ds(pl.multiple_of(j * width, width), width)
                part = jnp.dot(x_ref[:, k * chunk:(k + 1) * chunk], held[k % slots, :, here], preferred_element_type=F32)
                if k:
                    part = part + o_ref[:, here]
                o_ref[:, here] = part

            if k + slots < steps:
                fetch(k + slots).start()

    out = jax.ShapeDtypeStruct((x.shape[0], half), F32)
    scratch = [pltpu.VMEM((slots, chunk, half), BF16), pltpu.SemaphoreType.DMA((slots,))]
    return local_call(body, name, [x, w], out, 2 * x.shape[0] * depth * half, scratch=scratch, vmem=12, in_hbm=(1,))


def product(x, w, acc, dtype, depth_at, width_at, transposed, name):
    depth = x.shape[1]
    width = w.shape[0 if transposed else 1]
    if width_at is not None:
        width //= 2
    step = tile_of(width, 1024)

    def body(x_ref, w_ref, *rest):
        *acc_ref, o_ref = rest
        deep = pl.ds(half_start(*depth_at[:2], depth, depth_at[2]), depth)
        base = 0 if width_at is None else half_start(*width_at[:2], width, width_at[2])

        @pl.loop(0, width // step)
        def _(j):
            there = pl.ds(pl.multiple_of(base + j * step, step), step)
            here = pl.ds(pl.multiple_of(j * step, step), step)
            if transposed:
                part = lax.dot_general(x_ref[...], w_ref[there, deep], NT, preferred_element_type=F32)
            else:
                part = jnp.dot(x_ref[...], w_ref[deep, there], preferred_element_type=F32)
            if acc_ref:
                part = part + acc_ref[0][:, there]
            o_ref[:, here] = part.astype(dtype)

    out = jax.ShapeDtypeStruct((x.shape[0], width), dtype)
    arrays = [x, w] + ([] if acc is None else [acc])
    return local_call(body, name, arrays, out, 2 * x.shape[0] * depth * width)


def squares_of(w, far):
    rows, cols = w.shape
    half = rows // 2
    step = tile_of(half, 128)

    def body(w_ref, o_ref):
        for other in (False, True):
            start = half_start("narrow", far, half, other)

            @pl.loop(0, half // step)
            def _(j):
                here = pl.multiple_of(j * step, step)
                there = pl.ds(pl.multiple_of(start + here, step), step)
                total = jnp.zeros((step, 128), F32)
                for c in range(cols // 128):
                    part = w_ref[there, c * 128:(c + 1) * 128].astype(F32)
                    total = total + part * part
                o_ref[int(other):int(other) + 1, pl.ds(here, step)] = jnp.sum(total.T, axis=0, keepdims=True)

    out = jax.ShapeDtypeStruct((2, half), F32)
    return local_call(body, "squares", [w], out, 2 * 16 * rows * cols)


def finish(own, other, far):
    half = own.shape[1]

    def body(own_ref, other_ref, o_ref):
        o_ref[:, pl.ds(half_start("narrow", far, half, False), half)] = own_ref[...]
        o_ref[:, pl.ds(half_start("narrow", far, half, True), half)] = other_ref[...]

    out = jax.ShapeDtypeStruct((own.shape[0], 2 * half), F32)
    return local_call(body, "finish", [own, other], out, 1 << 10)


def local(harvest, pair_ids, w_enc, b_enc, w_dec, b_dec, step_size, penalty):
    rows = pair_ids.shape[0]
    lat, feat = w_dec.shape
    wide_bits, narrow_bits = bits_of("wide"), bits_of("narrow")
    far, near = narrow_bits[-1], narrow_bits[:-1]
    hidden, open_bits = wide_bits[0], wide_bits[1:]
    lat_own, lat_other = ("narrow", far, False), ("narrow", far, True)
    feat_own, feat_other = ("wide", hidden, False), ("wide", hidden, True)
    w_dec = pltpu.with_memory_space_constraint(w_dec, pltpu.VMEM)

    w_enc = pltpu.with_memory_space_constraint(w_enc, pltpu.HBM)
    pairs, step_row, pen_row = select(harvest, pair_ids, step_size, penalty, lat // 2, w_enc)
    for bit in wide_bits[:-1]:
        pairs = merge(pairs, swap(pairs, "wide", bit), w_enc)
    held = hold(w_dec, pen_row)
    pairs, pairs_own, b_enc_own, b_dec_own, step_row, pen_row = order(
        pairs, swap(pairs, "wide", wide_bits[-1]), b_enc[None], b_dec[None], step_row, pen_row, held, rows, far, hidden
    )
    batch = pairs.shape[0]
    wide_f32 = jax.ShapeDtypeStruct((batch, lat // 2), F32)
    lat_bf16 = jax.ShapeDtypeStruct((batch, lat // 2), BF16)
    feat_bf16 = jax.ShapeDtypeStruct((batch, feat // 2), BF16)

    def add_near(value, name):
        for bit in near:
            (value,) = pointwise(lambda a, b: (a + b,), name, [value, swap(value, "narrow", bit)], [jax.ShapeDtypeStruct(value.shape, F32)], w_dec)
        return value

    got = swap(encode(pairs, w_enc, far, True, "enc_other"), "narrow", far)
    (pre,) = pointwise(lambda a, b: (a + b,), "pre", [encode(pairs, w_enc, far, False, "enc_own"), got], [wide_f32], w_dec)
    for bit in near[:-1]:
        pre = pre + swap(pre, "narrow", bit)
    last = swap(pre, "narrow", near[-1])

    def first_codes(a, b, bias):
        value = jnp.maximum(a + b + bias, 0.0)
        return value, value.astype(BF16)

    latents, codes = pointwise(first_codes, "latents", [pre, last, b_enc_own], [wide_f32, lat_bf16], w_dec)

    half_row = jax.ShapeDtypeStruct((1, lat // 2), F32)
    two_rows = jax.ShapeDtypeStruct((2, lat // 2), F32)
    norms = squares_of(w_dec, far)
    for bit in near[:-1]:
        (norms,) = pointwise(lambda a, b: (a + b,), "squared", [norms, swap(norms, "narrow", bit)], [two_rows], w_dec)

    def roots(a, b):
        value = jnp.sqrt(a + b)
        return value[:1], value[1:]

    norm_own, norm_other = pointwise(roots, "norms", [norms, swap(norms, "narrow", near[-1])], [half_row, half_row], w_dec)
    norm_got = swap(norm_other, "narrow", far)

    for step in range(ITERS):
        codes_other = swap(codes, "narrow", far)
        acc = product(codes, w_dec, None, F32, lat_own, None, False, f"rebuild_a{step}")
        send = product(codes_other, w_dec, acc, BF16, lat_other, feat_other, False, f"rebuild_b{step}")
        got = swap(send, "wide", hidden)
        mine = product(codes_other, w_dec, acc, F32, lat_other, feat_own, False, f"rebuild_c{step}")
        for bit in open_bits:
            (mine,) = pointwise(lambda a, b: ((a.astype(F32) + b.astype(F32)).astype(BF16),), f"rebuilt{step}", [mine, got], [feat_bf16], w_dec)
            got = swap(mine, "wide", bit)

        def rest(mine, got, own, bias):
            return ((own.astype(F32) - (mine.astype(F32) + got.astype(F32)) - bias).astype(BF16),)

        (residual,) = pointwise(rest, f"residual{step}", [mine, got, pairs_own, b_dec_own], [feat_bf16], w_dec)
        residual_other = swap(residual, "wide", hidden)
        acc = product(residual, w_dec, None, F32, feat_own, None, True, f"grad_a{step}")
        send = product(residual_other, w_dec, acc, BF16, feat_other, lat_other, True, f"grad_b{step}")
        got = swap(send, "narrow", far)
        grad = product(residual_other, w_dec, acc, F32, feat_other, lat_own, True, f"grad_c{step}")
        for bit in near:
            (grad,) = pointwise(lambda a, b: (a + b.astype(F32),), f"grad{step}", [grad, got], [wide_f32], w_dec)
            got = swap(grad, "narrow", bit)

        def update(latents, grad, got, step_row, pen_row, norm_a, norm_b):
            thresh = pen_row * (norm_a + norm_b)
            value = jnp.maximum(latents + step_row * (grad + got.astype(F32)) - thresh, 0.0)
            return value, value.astype(BF16)

        latents, codes = pointwise(update, f"update{step}", [latents, grad, got, step_row, pen_row, norm_own, norm_got], [wide_f32, lat_bf16], w_dec)
    return finish(latents, swap(latents, "narrow", far), far)


def solution(mesh):
    return jax.shard_map(
        local,
        mesh=mesh,
        in_specs=(
            P("wide", "narrow"),
            P("wide"),
            P("narrow", "wide"),
            P("wide"),
            P("wide", "narrow"),
            P("narrow"),
            P(),
            P(),
        ),
        out_specs=P(None, "wide"),
        check_vma=False,
    )
```

```python
import functools

import jax
import jax.numpy as jnp
from jax import lax
from jax.experimental import pallas as pl
from jax.experimental.pallas import tpu as pltpu
from jax.sharding import PartitionSpec as P

ITERS = 2
MIB = 1024 * 1024
F32 = jnp.float32
BF16 = jnp.bfloat16
NT = (((1,), (1,)), ((), ()))


def swap(value, axis, distance):
    pairs = [(i, i ^ distance) for i in range(lax.axis_size(axis))]
    return lax.ppermute(value, axis, pairs)


def bits_of(axis):
    size = lax.axis_size(axis)
    assert size & (size - 1) == 0
    return [1 << k for k in range(size.bit_length() - 1)]


def tile_of(length, most):
    size = most
    while length % size:
        size //= 2
    return size


def half_start(axis, bit, half, other):
    high = jnp.where((lax.axis_index(axis) & bit) != 0, 1, 0)
    start = (1 - high if other else high) * half
    return pl.multiple_of(start, half)


def local_call(body, name, arrays, outs, flops, scalars=(), scratch=(), vmem=16, in_hbm=(), traffic=None):
    specs = [pl.BlockSpec(memory_space=pltpu.SMEM)] * len(scalars)
    specs += [pl.BlockSpec(memory_space=pltpu.HBM if k in in_hbm else pltpu.VMEM) for k in range(len(arrays))]
    multiple = isinstance(outs, (list, tuple))
    out_spec = pl.BlockSpec(memory_space=pltpu.VMEM)
    return pl.pallas_call(
        body,
        out_shape=outs,
        in_specs=specs,
        out_specs=[out_spec] * len(outs) if multiple else out_spec,
        scratch_shapes=list(scratch),
        compiler_params=pltpu.CompilerParams(vmem_limit_bytes=vmem * MIB),
        cost_estimate=pl.CostEstimate(flops=flops, bytes_accessed=flops // 32 if traffic is None else traffic, transcendentals=0),
        name=name,
    )(*scalars, *arrays)


def select(harvest, pair_ids, step_size, penalty, half_lat, w_enc):
    pool, feat = harvest.shape
    rows = pair_ids.shape[0]

    def body(step_ref, pen_ref, ids_ref, pool_ref, _, o_ref, step_row, pen_row):
        row = lax.broadcasted_iota(jnp.int32, (rows, pool), 0)
        col = lax.broadcasted_iota(jnp.int32, (rows, pool), 1)
        taken = jnp.zeros((rows, pool), F32)
        for r in range(rows):
            taken = jnp.where((row == r) & (col == ids_ref[r]), 1.0, taken)
        taken = taken.astype(BF16)
        chunk = tile_of(feat, 1024)

        @pl.loop(0, feat // chunk)
        def _(j):
            here = pl.ds(pl.multiple_of(j * chunk, chunk), chunk)
            o_ref[:, here] = jnp.dot(taken, pool_ref[:, here], preferred_element_type=F32).astype(BF16)

        step_row[...] = jnp.full((1, half_lat), step_ref[0, 0], F32)
        pen_row[...] = jnp.full((1, half_lat), pen_ref[0, 0] * step_ref[0, 0], F32)

    outs = [
        jax.ShapeDtypeStruct((rows, feat), BF16),
        jax.ShapeDtypeStruct((1, half_lat), F32),
        jax.ShapeDtypeStruct((1, half_lat), F32),
    ]
    scalars = [step_size.reshape(1, 1), penalty.reshape(1, 1), pair_ids]
    return local_call(body, "select", [harvest, w_enc], outs, 1 << 20, scalars, vmem=4, in_hbm=(1,))


def merge(mine, other, w_enc):
    count, feat = mine.shape

    def body(mine_ref, other_ref, _, o_ref):
        both = jnp.concatenate([mine_ref[...].astype(F32), other_ref[...].astype(F32)])
        o_ref[...] = both.astype(BF16)

    out = jax.ShapeDtypeStruct((2 * count, feat), BF16)
    return local_call(body, "merge", [mine, other, w_enc], out, 1 << 20, vmem=4, in_hbm=(2,))


def hold(w_dec, after):
    def body(w_ref, after_ref, o_ref):
        o_ref[...] = jnp.zeros(o_ref.shape, F32)

    out = jax.ShapeDtypeStruct((8, 128), F32)
    return local_call(body, "hold", [w_dec, pltpu.with_memory_space_constraint(after, pltpu.HBM)], out, 1 << 10, in_hbm=(1,))


def order(mine, other, b_enc, b_dec, step_row, pen_row, held, rows, far, hidden):
    count, feat = mine.shape
    half_feat, half_lat = feat // 2, b_enc.shape[1] // 2

    def body(mine_ref, other_ref, b_enc_ref, b_dec_ref, step_ref, pen_ref, _, all_ref, own_ref, enc_ref, dec_ref, step_out, pen_out):
        me = lax.axis_index("wide")
        row = lax.broadcasted_iota(jnp.int32, (2 * count, count), 0)
        col = lax.broadcasted_iota(jnp.int32, (2 * count, count), 1)

        def place(base):
            at = col + base
            return (row == rows * (me ^ (at // rows)) + at % rows).astype(F32).astype(BF16)

        chunk = tile_of(half_feat, 1024)
        start = half_start("wide", hidden, half_feat, False)

        @pl.loop(0, feat // chunk)
        def _(j):
            here = pl.ds(pl.multiple_of(j * chunk, chunk), chunk)
            both = jnp.dot(place(0), mine_ref[:, here], preferred_element_type=F32)
            both = both + jnp.dot(place(count), other_ref[:, here], preferred_element_type=F32)
            all_ref[:, here] = both.astype(BF16)

        own_ref[...] = all_ref[:, pl.ds(start, half_feat)]
        dec_ref[...] = b_dec_ref[:, pl.ds(start, half_feat)]
        enc_ref[...] = b_enc_ref[:, pl.ds(half_start("narrow", far, half_lat, False), half_lat)]
        step_out[...] = step_ref[...]
        pen_out[...] = pen_ref[...]

    outs = [
        jax.ShapeDtypeStruct((2 * count, feat), BF16),
        jax.ShapeDtypeStruct((2 * count, half_feat), BF16),
        jax.ShapeDtypeStruct((1, half_lat), F32),
        jax.ShapeDtypeStruct((1, half_feat), F32),
        jax.ShapeDtypeStruct((1, half_lat), F32),
        jax.ShapeDtypeStruct((1, half_lat), F32),
    ]
    return local_call(body, "order", [mine, other, b_enc, b_dec, step_row, pen_row, held], outs, 1 << 20, vmem=4)


def pointwise(fn, name, arrays, outs, w_dec):
    def body(*refs):
        ins, out_refs = refs[:len(arrays)], refs[len(arrays) + 1:]
        values = fn(*(ref[...] for ref in ins))
        for ref, value in zip(out_refs, values, strict=True):
            ref[...] = value

    return local_call(body, name, [*arrays, w_dec], outs, 1 << 16)


def encode(x, w, w_dec, far, other, name):
    depth, lat = w.shape
    half = lat // 2
    chunk = tile_of(depth, 256)
    steps = depth // chunk
    slots = min(8, steps)
    block = tile_of(half, 128)
    blocks = half // block

    def body(x_ref, w_ref, dec_ref, o_ref, sq_ref, held, sems):
        start = half_start("narrow", far, half, other)

        def fetch(k):
            return pltpu.make_async_copy(
                w_ref.at[pl.ds(k * chunk, chunk), pl.ds(start, half)], held.at[k % slots], sems.at[k % slots]
            )

        for k in range(slots):
            fetch(k).start()
        for k in range(steps):
            fetch(k).wait()
            part = jnp.dot(x_ref[:, k * chunk:(k + 1) * chunk], held[k % slots], preferred_element_type=F32)
            o_ref[...] = part + o_ref[...] if k else part
            for b in range(blocks):
                if b * steps // blocks == k:
                    there = pl.ds(pl.multiple_of(start + b * block, block), block)
                    total = jnp.zeros((block, 128), F32)
                    for c in range(dec_ref.shape[1] // 128):
                        value = dec_ref[there, c * 128:(c + 1) * 128].astype(F32)
                        total = total + value * value
                    sq_ref[:, b * block:(b + 1) * block] = jnp.sum(total.T, axis=0, keepdims=True)
            if k + slots < steps:
                fetch(k + slots).start()

    outs = [jax.ShapeDtypeStruct((x.shape[0], half), F32), jax.ShapeDtypeStruct((1, half), F32)]
    scratch = [pltpu.VMEM((slots, chunk, half), BF16), pltpu.SemaphoreType.DMA((slots,))]
    return local_call(body, name, [x, w, w_dec], outs, 2 * x.shape[0] * depth * half, scratch=scratch, in_hbm=(1,))


def product(x, w, acc, dtype, depth_at, width_at, transposed, name, after=()):
    depth = x.shape[1]
    width = w.shape[0 if transposed else 1]
    if width_at is not None:
        width //= 2
    step = tile_of(width, 1024)

    def body(x_ref, w_ref, *rest):
        acc_ref, o_ref = rest[:0 if acc is None else 1], rest[-1]
        deep = pl.ds(half_start(*depth_at[:2], depth, depth_at[2]), depth)
        base = 0 if width_at is None else half_start(*width_at[:2], width, width_at[2])

        @pl.loop(0, width // step)
        def _(j):
            there = pl.ds(pl.multiple_of(base + j * step, step), step)
            here = pl.ds(pl.multiple_of(j * step, step), step)
            if transposed:
                part = lax.dot_general(x_ref[...], w_ref[there, deep], NT, preferred_element_type=F32)
            else:
                part = jnp.dot(x_ref[...], w_ref[deep, there], preferred_element_type=F32)
            if acc_ref:
                part = part + acc_ref[0][:, there]
            o_ref[:, here] = part.astype(dtype)

    out = jax.ShapeDtypeStruct((x.shape[0], width), dtype)
    arrays = [x, w] + ([] if acc is None else [acc]) + list(after)
    return local_call(body, name, arrays, out, 2 * x.shape[0] * depth * width)


def finish(own, other, far):
    half = own.shape[1]

    def body(own_ref, other_ref, o_ref):
        o_ref[:, pl.ds(half_start("narrow", far, half, False), half)] = own_ref[...]
        o_ref[:, pl.ds(half_start("narrow", far, half, True), half)] = other_ref[...]

    out = jax.ShapeDtypeStruct((own.shape[0], 2 * half), F32)
    return local_call(body, "finish", [own, other], out, 1 << 10)


def local(harvest, pair_ids, w_enc, b_enc, w_dec, b_dec, step_size, penalty):
    rows = pair_ids.shape[0]
    lat, feat = w_dec.shape
    wide_bits, narrow_bits = bits_of("wide"), bits_of("narrow")
    far, near = narrow_bits[-1], narrow_bits[:-1]
    hidden, open_bits = wide_bits[0], wide_bits[1:]
    lat_own, lat_other = ("narrow", far, False), ("narrow", far, True)
    feat_own, feat_other = ("wide", hidden, False), ("wide", hidden, True)
    w_dec = pltpu.with_memory_space_constraint(w_dec, pltpu.VMEM)

    w_enc = pltpu.with_memory_space_constraint(w_enc, pltpu.HBM)
    pairs, step_row, pen_row = select(harvest, pair_ids, step_size, penalty, lat // 2, w_enc)
    for bit in wide_bits[:-1]:
        pairs = merge(pairs, swap(pairs, "wide", bit), w_enc)
    held = hold(w_dec, pen_row)
    pairs, pairs_own, b_enc_own, b_dec_own, step_row, pen_row = order(
        pairs, swap(pairs, "wide", wide_bits[-1]), b_enc[None], b_dec[None], step_row, pen_row, held, rows, far, hidden
    )
    batch = pairs.shape[0]
    wide_f32 = jax.ShapeDtypeStruct((batch, lat // 2), F32)
    lat_bf16 = jax.ShapeDtypeStruct((batch, lat // 2), BF16)
    feat_bf16 = jax.ShapeDtypeStruct((batch, feat // 2), BF16)

    def add_near(value, name):
        for bit in near:
            (value,) = pointwise(lambda a, b: (a + b,), name, [value, swap(value, "narrow", bit)], [jax.ShapeDtypeStruct(value.shape, F32)], w_dec)
        return value

    send, squares_other = encode(pairs, w_enc, w_dec, far, True, "enc_other")
    got = swap(send, "narrow", far)
    mine, squares_own = encode(pairs, w_enc, w_dec, far, False, "enc_own")
    (pre,) = pointwise(lambda a, b: (a + b,), "pre", [mine, got], [wide_f32], w_dec)
    for bit in near[:-1]:
        pre = pre + swap(pre, "narrow", bit)
    last = swap(pre, "narrow", near[-1])

    half_row = jax.ShapeDtypeStruct((1, lat // 2), F32)
    two_rows = jax.ShapeDtypeStruct((2, lat // 2), F32)
    (norms,) = pointwise(lambda a, b: (jnp.concatenate([a, b]),), "squares", [squares_own, squares_other], [two_rows], w_dec)
    for bit in near[:-1]:
        (norms,) = pointwise(lambda a, b: (a + b,), "squared", [norms, swap(norms, "narrow", bit)], [two_rows], w_dec)

    def roots(a, b):
        value = jnp.sqrt(a + b)
        return value[:1], value[1:]

    norm_own, norm_other = pointwise(roots, "norms", [norms, swap(norms, "narrow", near[-1])], [half_row, half_row], w_dec)
    norm_got = swap(norm_other, "narrow", far)

    def first_codes(a, b, bias, _):
        value = jnp.maximum(a + b + bias, 0.0)
        return value, value.astype(BF16)

    latents, codes = pointwise(first_codes, "latents", [pre, last, b_enc_own, norm_other], [wide_f32, lat_bf16], w_dec)

    for step in range(ITERS):
        codes_other = swap(codes, "narrow", far)
        acc = product(codes, w_dec, None, F32, lat_own, None, False, f"rebuild_a{step}")
        send = product(codes_other, w_dec, acc, BF16, lat_other, feat_other, False, f"rebuild_b{step}", after=[norm_got])
        got = swap(send, "wide", hidden)
        mine = product(codes_other, w_dec, acc, F32, lat_other, feat_own, False, f"rebuild_c{step}")
        for bit in open_bits:
            (mine,) = pointwise(lambda a, b: ((a.astype(F32) + b.astype(F32)).astype(BF16),), f"rebuilt{step}", [mine, got], [feat_bf16], w_dec)
            got = swap(mine, "wide", bit)

        def rest(mine, got, own, bias):
            return ((own.astype(F32) - (mine.astype(F32) + got.astype(F32)) - bias).astype(BF16),)

        (residual,) = pointwise(rest, f"residual{step}", [mine, got, pairs_own, b_dec_own], [feat_bf16], w_dec)
        residual_other = swap(residual, "wide", hidden)
        acc = product(residual, w_dec, None, F32, feat_own, None, True, f"grad_a{step}")
        send = product(residual_other, w_dec, acc, BF16, feat_other, lat_other, True, f"grad_b{step}")
        got = swap(send, "narrow", far)
        grad = product(residual_other, w_dec, acc, F32, feat_other, lat_own, True, f"grad_c{step}")
        for bit in near:
            (grad,) = pointwise(lambda a, b: (a + b.astype(F32),), f"grad{step}", [grad, got], [wide_f32], w_dec)
            got = swap(grad, "narrow", bit)

        def update(latents, grad, got, step_row, pen_row, norm_a, norm_b):
            thresh = pen_row * (norm_a + norm_b)
            value = jnp.maximum(latents + step_row * (grad + got.astype(F32)) - thresh, 0.0)
            return value, value.astype(BF16)

        latents, codes = pointwise(update, f"update{step}", [latents, grad, got, step_row, pen_row, norm_own, norm_got], [wide_f32, lat_bf16], w_dec)
    return finish(latents, swap(latents, "narrow", far), far)


def solution(mesh):
    return jax.shard_map(
        local,
        mesh=mesh,
        in_specs=(
            P("wide", "narrow"),
            P("wide"),
            P("narrow", "wide"),
            P("wide"),
            P("wide", "narrow"),
            P("narrow"),
            P(),
            P(),
        ),
        out_specs=P(None, "wide"),
        check_vma=False,
    )
```
